32 devices in a mesh: dp: 4 (over x, y), tp: 8 (over z, core).
Axes of the slice: x: 2, y: 2, z: 4, core: 2. Of those that a mesh axis runs over, the one named last changes fastest.
Arguments:
- x: bfloat16 [8192, 3072], P('dp'), parts along dimension 0
- dy: bfloat16 [8192, 3072], P('dp'), parts along dimension 0
- gate: bfloat16 [8192, 8192], P('dp', 'tp'), parts along dimension 0
- up: bfloat16 [8192, 8192], P('dp', 'tp'), parts along dimension 0
- w_gate: bfloat16 [3072, 8192], P(None, 'tp')
- w_up: bfloat16 [3072, 8192], P(None, 'tp')
- w_down: bfloat16 [8192, 3072], P('tp')
Outputs:
- output 1: bfloat16 [8192, 3072], P('dp'), parts along dimension 0
- output 2: bfloat16 [12288, 8192], P('dp', 'tp'), parts along dimension 0
- output 3: bfloat16 [12288, 8192], P('dp', 'tp'), parts along dimension 0
- output 4: bfloat16 [32768, 3072], P(('dp', 'tp')), parts along dimension 0
There are 4 independent parts. The reference program is written for one: setup_inputs(seed, part) draws one part's arguments, and reference() takes and returns one part's arrays. A program takes and returns all parts, laid end to end along the dimension named above; an argument that names none is the same for every part.
All inputs are finite; a program needn't handle non-finite values.
Results may differ from the reference program's by a relative error of at most 0.012.
Values are sent between devices in bfloat16 or wider.
A program may use at most 2 GiB of HBM per device.

```python
import jax
import jax.numpy as jnp

ROWS = 2048
D = 3072
FF = 8192


def act(gate, up):
    return jax.nn.silu(gate) * up


def setup_inputs(seed: int = 0, part: int = 0) -> dict:
    kx, ky, ka, kb, kg, ku, kd = jax.random.split(jax.random.key(seed), 7)
    kx, ky, ka, kb = (jax.random.fold_in(k, part) for k in (kx, ky, ka, kb))
    drawn = {
        "x": jax.random.normal(kx, (ROWS, D), jnp.float32),
        "dy": jax.random.normal(ky, (ROWS, D), jnp.float32),
        "gate": jax.random.normal(ka, (ROWS, FF), jnp.float32),
        "up": jax.random.normal(kb, (ROWS, FF), jnp.float32),
        "w_gate": jax.random.normal(kg, (D, FF), jnp.float32) * D**-0.5,
        "w_up": jax.random.normal(ku, (D, FF), jnp.float32) * D**-0.5,
        "w_down": jax.random.normal(kd, (FF, D), jnp.float32) * FF**-0.5,
    }
    return {k: v.astype(jnp.bfloat16) for k, v in drawn.items()}


def reference(x, dy, gate, up, w_gate, w_up, w_down):
    hidden, back = jax.vjp(act, gate.astype(jnp.float32), up.astype(jnp.float32))
    d_hidden = jnp.dot(dy, w_down.T, preferred_element_type=jnp.float32)
    d_gate, d_up = (g.astype(jnp.bfloat16) for g in back(d_hidden))
    dx = jnp.dot(d_gate, w_gate.T, preferred_element_type=jnp.float32) + jnp.dot(d_up, w_up.T, preferred_element_type=jnp.float32)
    dw_gate = jnp.dot(x.T, d_gate, preferred_element_type=jnp.float32)
    dw_up = jnp.dot(x.T, d_up, preferred_element_type=jnp.float32)
    dw_down = jnp.dot(hidden.astype(jnp.bfloat16).T, dy, preferred_element_type=jnp.float32)
    return tuple(g.astype(jnp.bfloat16) for g in (dx, dw_gate, dw_up, dw_down))
```

```python
import functools

import jax
import jax.numpy as jnp
from jax import lax
from jax.experimental import pallas as pl
from jax.experimental.pallas import tpu as pltpu
from jax.sharding import PartitionSpec as P

MESH = pl.DeviceIdType.MESH
F32, BF16 = jnp.float32, jnp.bfloat16
ROWS, D, FL = 2048, 3072, 1024
BLK, HALF, CT = 512, 256, 512
NB, NJ = ROWS // BLK, D // CT
NU = NB * NJ
NIN = 4
NT = (((1,), (1,)), ((), ()))
NN = (((1,), (0,)), ((), ()))


def dot(a, b, dims):
    return lax.dot_general(a, b, dims, preferred_element_type=F32)


def m(i, n):
    return pl.multiple_of(i * n, n)


def kernel(comm, x, dy, gate, up, wg, wu, wd, dx, dwg, dwu, dwd,
           wgu_v, wd_v, dgu, hid, dyb, gb, ub, A, B, Q, d_out, d_in,
           w_sem, in_sem, x_sem, y_sem, o_sem, p_sem,
           d_send, d_recv, s1, r1, r2, s3, s4, r4, s5, credit):
    tp = lax.axis_index("tp")
    z, c = tp // 2, lax.rem(tp, 2)
    inner = jnp.logical_and(z >= 1, z <= 2)
    outer = jnp.logical_not(inner)
    sib = z * 2 + (1 - c)
    line = jnp.where(z == 0, 1, jnp.where(z == 1, 0, jnp.where(z == 2, 3, 2))) * 2 + c
    mid = (3 - z) * 2 + c

    def loads(b, pairs):
        out = []
        for h in range(2):
            src = pl.multiple_of(b * BLK + (c if h == 0 else 1 - c) * HALF, HALF)
            rows, dst = pl.ds(src, HALF), pl.ds(h * HALF, HALF)
            for i, src_ref, dst_ref in pairs:
                out.append(pltpu.make_async_copy(src_ref.at[rows, :], dst_ref.at[dst, :], in_sem.at[i + h]))
        return out

    def dy_loads(b):
        return loads(b, [(0, dy, dyb)])

    def gu_loads(b):
        return loads(b, [(2, gate, gb), (4, up, ub)])

    wd_load = pltpu.make_async_copy(wd, wd_v, w_sem.at[0])
    wg_load = pltpu.make_async_copy(wg, wgu_v.at[:, pl.ds(0, FL)], w_sem.at[1])
    wu_load = pltpu.make_async_copy(wu, wgu_v.at[:, pl.ds(FL, FL)], w_sem.at[2])
    for cp in dy_loads(0):
        cp.start()
    wd_load.start()
    for cp in gu_loads(0):
        cp.start()
    wg_load.start()
    wu_load.start()

    if comm:
        barrier = pltpu.get_barrier_semaphore()
        pl.semaphore_signal(barrier, inc=1, device_id={"tp": sib}, device_id_type=MESH)
        pl.semaphore_signal(barrier, inc=1, device_id={"tp": line}, device_id_type=MESH)

        @pl.when(inner)
        def _():
            pl.semaphore_signal(barrier, inc=1, device_id={"tp": mid}, device_id_type=MESH)
            pl.semaphore_wait(barrier, 3)

        @pl.when(outer)
        def _():
            pl.semaphore_wait(barrier, 2)

    def remote(src, dst, send, recv, to):
        return pltpu.make_async_remote_copy(
            src_ref=src, dst_ref=dst, send_sem=send, recv_sem=recv, device_id={"tp": to}, device_id_type=MESH)

    def d_copy(u):
        return remote(d_out.at[lax.rem(u, 2)], d_in.at[lax.rem(u, NIN)], d_send.at[lax.rem(u, 2)],
                      d_recv.at[lax.rem(u, NIN)], sib)

    def p_copy(u):
        return remote(A.at[u], A.at[u], s1.at[u], r1.at[u], line)

    def q_copy(u):
        return remote(A.at[u], Q.at[u], s1.at[u], r2.at[u], mid)

    def piece(u, core):
        b, j = u // NJ, lax.rem(u, NJ)
        return dx.at[pl.ds(pl.multiple_of(b * BLK + core * HALF, HALF), HALF), pl.ds(m(j, CT), CT)]

    def f_copy(u):
        return remote(A.at[u], piece(u, c), s3.at[u], r2.at[u], line)

    def g_copy(u, src):
        return remote(src, piece(u, c), s4.at[u], r4.at[u], sib)

    def l_copy(u):
        return pltpu.make_async_copy(A.at[u], piece(u, c), s5.at[u])

    def when(cond):
        return pl.when(cond)

    def take_sibling(u):
        d_copy(u).wait_recv()

        @when(outer)
        def _():
            A[u] = (B[u] + d_in[lax.rem(u, NIN)].astype(F32)).astype(BF16)
            p_copy(u).start()

        @when(inner)
        def _():
            B[u] = B[u] + d_in[lax.rem(u, NIN)].astype(F32)

        @when(u < NU - NIN)
        def _():
            pl.semaphore_signal(credit, inc=1, device_id={"tp": sib}, device_id_type=MESH)

    def inner_sum(u):
        p_copy(u).wait_recv()
        A[u] = (B[u] + A[u].astype(F32)).astype(BF16)
        q_copy(u).start()

    def final_sum(u):
        q_copy(u).wait_recv()
        q_copy(u).wait_send()
        A[u] = (A[u].astype(F32) + Q[u].astype(F32)).astype(BF16)
        f_copy(u).start()
        g_copy(u, A.at[u]).start()
        l_copy(u).start()

    def forward(u):
        f_copy(u).wait_recv()
        g_copy(u, piece(u, c)).start()

    def tick(h):
        if not comm:
            return

        @when(jnp.logical_and(inner, jnp.logical_and(h >= 2, h < NU + 2)))
        def _():
            inner_sum(h - 2)

        @when(jnp.logical_and(inner, jnp.logical_and(h >= 4, h < NU + 4)))
        def _():
            final_sum(h - 4)

        @when(jnp.logical_and(outer, jnp.logical_and(h >= 6, h < NU + 6)))
        def _():
            forward(h - 6)

    def block(b, _):
        for cp in dy_loads(b):
            cp.wait()

        @when(b == 0)
        def _():
            wd_load.wait()

        for cp in gu_loads(b):
            cp.wait()

        def hidden(n, _):
            cols = pl.ds(m(n, 512), 512)
            dh = dot(dyb[...], wd_v[cols, :], NT)
            g, u = gb[:, cols].astype(F32), ub[:, cols].astype(F32)
            s = jax.nn.sigmoid(g)
            gs = g * s
            rows = pl.ds(m(b, BLK), BLK)
            dgu[rows, cols] = (dh * u * (s * (1.0 + g * (1.0 - s)))).astype(BF16)
            dgu[rows, pl.ds(pl.multiple_of(FL + n * 512, 512), 512)] = (dh * gs).astype(BF16)
            hid[cols, rows] = (gs * u).T.astype(BF16)
            return 0

        lax.fori_loop(0, FL // 512, hidden, 0)

        @when(b < NB - 1)
        def _():
            for cp in dy_loads(b + 1) + gu_loads(b + 1):
                cp.start()

        @when(b == 0)
        def _():
            wg_load.wait()
            wu_load.wait()

        def unit(j, _):
            u = b * NJ + j
            if comm:
                @when(u >= 2)
                def _():
                    d_copy(u - 2).wait_send()
            t = dot(dgu[pl.ds(m(b, BLK), BLK), :], wgu_v[pl.ds(m(j, CT), CT), :], NT)
            B[u] = t[:HALF]
            d_out[lax.rem(u, 2)] = t[HALF:].astype(BF16)
            if comm:
                @when(u >= NIN)
                def _():
                    pl.semaphore_wait(credit, 1)
                d_copy(u).start()

                @when(u >= 1)
                def _():
                    take_sibling(u - 1)

                @when(lax.rem(u, 2) == 1)
                def _():
                    tick(u // 2)
            return 0

        lax.fori_loop(0, NJ, unit, 0)
        return 0

    lax.fori_loop(0, NB, block, 0)
    if comm:
        take_sibling(NU - 1)

    def tile_copies(src, i, slot0, sem):
        slot = lax.rem(i, 2)
        cols = pl.ds(m(i, 512), 512)
        dst_cols = pl.ds(pl.multiple_of((slot0 + slot) * 512, 512), 512)
        return [
            pltpu.make_async_copy(
                src.at[pl.ds(pl.multiple_of(b * BLK + (c if h == 0 else 1 - c) * HALF, HALF), HALF), cols],
                wgu_v.at[pl.ds(b * BLK + h * HALF, HALF), dst_cols],
                sem.at[slot, 2 * b + h],
            )
            for b in range(NB)
            for h in range(2)
        ]

    def gu_out(i):
        slot = lax.rem(i, 2)
        rows = pl.ds(pl.multiple_of(2048 + slot * 512, 512), 512)
        dst = pl.ds(m(i, 512), 512)
        return (
            pltpu.make_async_copy(wgu_v.at[rows, pl.ds(0, FL)], dwg.at[dst, :], o_sem.at[0, slot]),
            pltpu.make_async_copy(wgu_v.at[rows, pl.ds(FL, FL)], dwu.at[dst, :], o_sem.at[1, slot]),
        )

    def down_out(i):
        slot = lax.rem(i, 2)
        return pltpu.make_async_copy(
            wd_v.at[:, pl.ds(m(slot, 512), 512)], dwd.at[:, pl.ds(m(i, 512), 512)], o_sem.at[2, slot])

    for cp in tile_copies(x, 0, 0, x_sem) + tile_copies(dy, 0, 2, y_sem):
        cp.start()
    NI = D // 512
    xt = dyb.at[:, pl.ds(0, ROWS)]

    def grads(i, _):
        slot = lax.rem(i, 2)

        @when(i + 1 < NI)
        def _():
            for cp in tile_copies(x, i + 1, 0, x_sem) + tile_copies(dy, i + 1, 2, y_sem):
                cp.start()

        for cp in tile_copies(x, i, 0, x_sem):
            cp.wait()

        @when(i >= 2)
        def _():
            for cp in gu_out(i - 2):
                cp.wait()
            down_out(i - 2).wait()

        xc = pl.ds(m(slot, 512), 512)

        def flip(r, _):
            rows = pl.ds(m(r, 512), 512)
            xt[:, rows] = wgu_v[rows, xc].T
            return 0

        lax.fori_loop(0, ROWS // 512, flip, 0)
        out_rows = pl.ds(pl.multiple_of(2048 + slot * 512, 512), 512)

        def gu(n, _):
            cols = pl.ds(m(n, 512), 512)
            wgu_v[out_rows, cols] = dot(xt[...], dgu[:, cols], NN).astype(BF16)

            @when(lax.rem(n, 2) == 1)
            def _():
                tick_p(i * 3 + n // 2)
            return 0

        lax.fori_loop(0, 4, gu, 0)
        for cp in gu_out(i):
            cp.start()
        for cp in tile_copies(dy, i, 2, y_sem):
            cp.wait()

        yc = pl.ds(pl.multiple_of((2 + slot) * 512, 512), 512)

        def down(n, _):
            rows = pl.ds(m(n, 512), 512)
            wd_v[rows, pl.ds(m(slot, 512), 512)] = dot(hid[rows, :], wgu_v[pl.ds(0, ROWS), yc], NN).astype(BF16)
            return 0

        lax.fori_loop(0, 2, down, 0)
        down_out(i).start()
        tick_p(i * 3 + 2)
        return 0

    def tick_p(p):
        @when(lax.rem(p, 2) == 1)
        def _():
            tick(NU // 2 + p // 2)

    lax.fori_loop(0, NI, grads, 0)
    for i in (NI - 2, NI - 1):
        for cp in gu_out(i):
            cp.wait()
        down_out(i).wait()

    if comm:
        def drain(h, _):
            tick(h)
            return 0

        lax.fori_loop(NU // 2 + 3 * NI // 2, NU + 6, drain, 0)
        d_copy(NU - 2).wait_send()
        d_copy(NU - 1).wait_send()

        def finish(u, _):
            g_copy(u, A.at[u]).wait()

            @when(outer)
            def _():
                p_copy(u).wait_send()

            @when(inner)
            def _():
                f_copy(u).wait_send()
                l_copy(u).wait()
            return 0

        lax.fori_loop(0, NU, finish, 0)


def fused(comm, *args):
    any_ = pl.BlockSpec(memory_space=pl.ANY)
    V, DMA = pltpu.VMEM, pltpu.SemaphoreType.DMA
    scratch = [
        V((D, 2 * FL), BF16), V((FL, D), BF16), V((ROWS, 2 * FL), BF16), V((FL, ROWS), BF16),
        V((BLK, D), BF16), V((BLK, FL), BF16), V((BLK, FL), BF16),
        V((NU, HALF, CT), BF16), V((NU, HALF, CT), F32), V((NU, HALF, CT), BF16),
        V((2, HALF, CT), BF16), V((NIN, HALF, CT), BF16),
        DMA((3,)), DMA((6,)), DMA((2, 8)), DMA((2, 8)), DMA((3, 2)), DMA((1,)),
        DMA((2,)), DMA((NIN,)), DMA((NU,)), DMA((NU,)), DMA((NU,)), DMA((NU,)), DMA((NU,)), DMA((NU,)), DMA((NU,)),
        pltpu.SemaphoreType.REGULAR,
    ]
    S = jax.ShapeDtypeStruct
    return pl.pallas_call(
        functools.partial(kernel, comm),
        out_shape=(S((ROWS, D), BF16), S((D, FL), BF16), S((D, FL), BF16), S((FL, D), BF16)),
        in_specs=[any_] * 7,
        out_specs=(any_,) * 4,
        scratch_shapes=scratch,
        cost_estimate=pl.CostEstimate(flops=12 * ROWS * D * FL, bytes_accessed=90_000_000, transcendentals=ROWS * FL),
        compiler_params=pltpu.CompilerParams(
            collective_id=0 if comm else None, has_side_effects=True, vmem_limit_bytes=67_043_328),
    )(*args)


def solution(mesh, comm=True):
    tokens, columns, rows = P("dp", None), P(None, "tp"), P("tp", None)
    return jax.shard_map(
        functools.partial(fused, comm),
        mesh=mesh,
        in_specs=(tokens, tokens, P("dp", "tp"), P("dp", "tp"), columns, columns, rows),
        out_specs=(tokens, P("dp", "tp"), P("dp", "tp"), P(("dp", "tp"), None)),
        check_vma=False,
    )
```

```python
import functools

import jax
import jax.numpy as jnp
from jax import lax
from jax.experimental import pallas as pl
from jax.experimental.pallas import tpu as pltpu
from jax.sharding import PartitionSpec as P

MESH = pl.DeviceIdType.MESH
F32, BF16 = jnp.float32, jnp.bfloat16
ROWS, D, FL = 2048, 3072, 1024
BLK, HALF, TILE, CT = 512, 256, 512, 256
NB, NJ = ROWS // BLK, D // TILE
NT_, NU = NB * NJ, NB * (D // CT)
PER = TILE // CT
NIN, NBUF = 4, 16
NT = (((1,), (1,)), ((), ()))
NN = (((1,), (0,)), ((), ()))


def dot(a, b, dims):
    return lax.dot_general(a, b, dims, preferred_element_type=F32)


def m(i, n):
    return pl.multiple_of(i * n, n)


def kernel(comm, x, dy, gate, up, wg, wu, wd, dx, dwg, dwu, dwd,
           dgu, hid, dyb, gb, ub, xv, yv, B, d_out, d_in,
           w_sem, in_sem, x_sem, y_sem,
           d_send, d_recv, s1, r1, r2, s3, s4, r4, credit, g_credit, f_credit):
    tp = lax.axis_index("tp")
    z, c = tp // 2, lax.rem(tp, 2)
    inner = jnp.logical_and(z >= 1, z <= 2)
    outer = jnp.logical_not(inner)
    sib = z * 2 + (1 - c)
    line = jnp.where(z == 0, 1, jnp.where(z == 1, 0, jnp.where(z == 2, 3, 2))) * 2 + c
    mid = (3 - z) * 2 + c

    def loads(b, pairs):
        out = []
        for h in range(2):
            src = pl.multiple_of(b * BLK + (c if h == 0 else 1 - c) * HALF, HALF)
            rows, dst = pl.ds(src, HALF), pl.ds(h * HALF, HALF)
            for i, src_ref, dst_ref in pairs:
                out.append(pltpu.make_async_copy(src_ref.at[rows, :], dst_ref.at[dst, :], in_sem.at[i + h]))
        return out

    def dy_loads(b):
        return loads(b, [(0, dy, dyb)])

    def gu_loads(b):
        return loads(b, [(2, gate, gb), (4, up, ub)])

    def wd_load(n):
        rows = pl.ds(m(n, 512), 512)
        return pltpu.make_async_copy(wd.at[rows, :], dwd.at[rows, :], w_sem.at[n])

    wg_load = pltpu.make_async_copy(wg, dwg, w_sem.at[2])
    wu_load = pltpu.make_async_copy(wu, dwu, w_sem.at[3])
    for cp in dy_loads(0):
        cp.start()
    wd_load(0).start()
    for cp in gu_loads(0):
        cp.start()
    wd_load(1).start()
    wg_load.start()
    wu_load.start()

    if comm:
        barrier = pltpu.get_barrier_semaphore()
        pl.semaphore_signal(barrier, inc=1, device_id={"tp": sib}, device_id_type=MESH)
        pl.semaphore_signal(barrier, inc=1, device_id={"tp": line}, device_id_type=MESH)

        @pl.when(inner)
        def _():
            pl.semaphore_signal(barrier, inc=1, device_id={"tp": mid}, device_id_type=MESH)
            pl.semaphore_wait(barrier, 3)

        @pl.when(outer)
        def _():
            pl.semaphore_wait(barrier, 2)

    def remote(src, dst, send, recv, to):
        return pltpu.make_async_remote_copy(
            src_ref=src, dst_ref=dst, send_sem=send, recv_sem=recv, device_id={"tp": to}, device_id_type=MESH)

    def at(u, core):
        n = D // CT
        b, j = u // n, lax.rem(u, n)
        return pl.ds(pl.multiple_of(b * BLK + core * HALF, HALF), HALF), pl.ds(m(j, CT), CT)

    def mine(u):
        return dx.at[*at(u, c)]

    def theirs(u):
        return dx.at[*at(u, 1 - c)]

    def d_copy(t):
        return remote(d_out.at[lax.rem(t, 2)], d_in.at[lax.rem(t, NIN)], d_send.at[lax.rem(t, 2)],
                      d_recv.at[lax.rem(t, NIN)], sib)

    def p_copy(u):
        return remote(mine(u), mine(u), s1.at[u], r1.at[u], line)

    def q_copy(u):
        return remote(mine(u), theirs(u), s1.at[u], r2.at[u], mid)

    def f_copy(u):
        return remote(mine(u), mine(u), s3.at[0], r2.at[u], line)

    def g_copy(u):
        return remote(mine(u), mine(u), s4.at[0], r4.at[0], sib)

    def pending(u):
        i = lax.rem(u, PER)
        return lax.rem(u // PER, NBUF), slice(None), pl.ds(m(i, CT), CT)

    def take_sibling(t):
        d_copy(t).wait_recv()
        b, j = t // NJ, lax.rem(t, NJ)
        total = B[lax.rem(t, NBUF)] + d_in[lax.rem(t, NIN)].astype(F32)

        @pl.when(outer)
        def _():
            dx[pl.ds(pl.multiple_of(b * BLK + c * HALF, HALF), HALF), pl.ds(m(j, TILE), TILE)] = total.astype(BF16)
            for i in range(PER):
                p_copy(t * PER + i).start()

        @pl.when(inner)
        def _():
            B[lax.rem(t, NBUF)] = total

        @pl.when(t < NT_ - NIN)
        def _():
            pl.semaphore_signal(credit, inc=1, device_id={"tp": sib}, device_id_type=MESH)

    def inner_sum(u):
        p_copy(u).wait_recv()
        p = at(u, c)
        dx[*p] = (B[*pending(u)] + dx[*p].astype(F32)).astype(BF16)
        q_copy(u).start()

    def final_sum(u):
        q_copy(u).wait_recv()
        q_copy(u).wait_send()
        p = at(u, c)
        dx[*p] = (dx[*p].astype(F32) + dx[*at(u, 1 - c)].astype(F32)).astype(BF16)
        pl.semaphore_signal(g_credit, inc=1, device_id={"tp": sib}, device_id_type=MESH)
        pl.semaphore_wait(f_credit, 1)
        f_copy(u).start()
        pl.semaphore_wait(g_credit, 1)
        g_copy(u).start()

    def release(u):
        p_copy(u).wait_send()
        pl.semaphore_signal(f_credit, inc=1, device_id={"tp": line}, device_id_type=MESH)

    def forward(u):
        f_copy(u).wait_recv()
        g_copy(u).start()

    def tick(h):
        if not comm:
            return

        @pl.when(jnp.logical_and(inner, jnp.logical_and(h >= LAG[0], h < NU + LAG[0])))
        def _():
            inner_sum(h - LAG[0])

        @pl.when(jnp.logical_and(inner, jnp.logical_and(h >= LAG[1], h < NU + LAG[1])))
        def _():
            final_sum(h - LAG[1])

        @pl.when(jnp.logical_and(outer, jnp.logical_and(h >= LAG[0], h < NU + LAG[0])))
        def _():
            release(h - LAG[0])

        @pl.when(jnp.logical_and(outer, jnp.logical_and(h >= LAG[2], h < NU + LAG[2])))
        def _():
            forward(h - LAG[2])

    def block(b, _):
        for cp in dy_loads(b):
            cp.wait()
        rows = pl.ds(m(b, BLK), BLK)

        def hidden(n, _):
            @pl.when(b == 0)
            def _():
                wd_load(n).wait()

            cols = pl.ds(m(n, 512), 512)
            dh = dot(dyb[...], dwd[cols, :], NT)

            @pl.when(n == 0)
            def _():
                for cp in gu_loads(b):
                    cp.wait()

            g, u = gb[:, cols].astype(F32), ub[:, cols].astype(F32)
            s = jax.nn.sigmoid(g)
            gs = g * s
            dgu[rows, cols] = (dh * u * (s * (1.0 + g * (1.0 - s)))).astype(BF16)
            dgu[rows, pl.ds(pl.multiple_of(FL + n * 512, 512), 512)] = (dh * gs).astype(BF16)
            hid[cols, rows] = (gs * u).T.astype(BF16)
            return 0

        lax.fori_loop(0, FL // 512, hidden, 0)

        @pl.when(b < NB - 1)
        def _():
            for cp in dy_loads(b + 1) + gu_loads(b + 1):
                cp.start()

        @pl.when(b == 0)
        def _():
            wg_load.wait()
            wu_load.wait()

        def tile(j, _):
            t = b * NJ + j
            if comm:
                @pl.when(t >= 2)
                def _():
                    d_copy(t - 2).wait_send()
            cols = pl.ds(m(j, TILE), TILE)
            v = dot(dgu[rows, pl.ds(0, FL)], dwg[cols, :], NT) + dot(dgu[rows, pl.ds(FL, FL)], dwu[cols, :], NT)
            B[lax.rem(t, NBUF)] = v[:HALF]
            d_out[lax.rem(t, 2)] = v[HALF:].astype(BF16)
            if comm:
                @pl.when(t >= NIN)
                def _():
                    pl.semaphore_wait(credit, 1)
                d_copy(t).start()

                @pl.when(t >= 1)
                def _():
                    take_sibling(t - 1)

                tick(t)
            return 0

        lax.fori_loop(0, NJ, tile, 0)
        return 0

    def tile_copies(src, dst, i, sem):
        cols = pl.ds(m(i, 512), 512)
        return [
            pltpu.make_async_copy(
                src.at[pl.ds(pl.multiple_of(b * BLK + (c if h == 0 else 1 - c) * HALF, HALF), HALF), cols],
                dst.at[pl.ds(b * BLK + h * HALF, HALF), :],
                sem.at[2 * b + h],
            )
            for b in range(NB)
            for h in range(2)
        ]

    for cp in tile_copies(x, xv, 0, x_sem) + tile_copies(dy, yv, 0, y_sem):
        cp.start()

    lax.fori_loop(0, NB, block, 0)
    if comm:
        take_sibling(NT_ - 1)

    NI = D // 512
    xt = dyb.at[:, pl.ds(0, ROWS)]

    def grads(i, _):
        for cp in tile_copies(x, xv, i, x_sem):
            cp.wait()

        def flip(r, _):
            rows = pl.ds(m(r, 512), 512)
            xt[:, rows] = xv[rows, :].T
            return 0

        lax.fori_loop(0, ROWS // 512, flip, 0)

        @pl.when(i + 1 < NI)
        def _():
            for cp in tile_copies(x, xv, i + 1, x_sem):
                cp.start()

        out = pl.ds(m(i, 512), 512)

        def gu(n, _):
            cols = pl.ds(m(n, 512), 512)
            dwg[out, cols] = dot(xt[...], dgu[:, cols], NN).astype(BF16)
            dwu[out, cols] = dot(xt[...], dgu[:, pl.ds(pl.multiple_of(FL + n * 512, 512), 512)], NN).astype(BF16)
            tick(NT_ + 4 * i + n)
            return 0

        lax.fori_loop(0, 2, gu, 0)
        for cp in tile_copies(dy, yv, i, y_sem):
            cp.wait()

        def down(n, _):
            rows = pl.ds(m(n, 512), 512)
            dwd[rows, out] = dot(hid[rows, :], yv[...], NN).astype(BF16)
            tick(NT_ + 4 * i + 2 + n)
            return 0

        lax.fori_loop(0, 2, down, 0)

        @pl.when(i + 1 < NI)
        def _():
            for cp in tile_copies(dy, yv, i + 1, y_sem):
                cp.start()
        return 0

    lax.fori_loop(0, NI, grads, 0)

    if comm:
        def drain(h, _):
            tick(h)
            return 0

        lax.fori_loop(NT_ + 4 * NI, NU + LAG[2], drain, 0)
        d_copy(NT_ - 2).wait_send()
        d_copy(NT_ - 1).wait_send()
        half = dx.at[pl.ds(0, ROWS // 2), :]
        remote(half, half, s4.at[0], r4.at[0], sib).wait()

        @pl.when(inner)
        def _():
            remote(half, half, s3.at[0], r2.at[0], line).wait_send()


def write(*refs):
    n = len(refs) // 2
    sem, refs = refs[-1], refs[:-1]
    copies = []
    for i in range(n):
        src, dst = refs[i], refs[n + i]
        rows = src.shape[0] // 4
        for k in range(4):
            part = pl.ds(k * rows, rows)
            copies.append(pltpu.make_async_copy(src.at[part, :], dst.at[part, :], sem.at[i, k]))
    for cp in copies:
        cp.start()
    for cp in copies:
        cp.wait()


SHAPES = ((ROWS, D), (D, FL), (D, FL), (FL, D))
LAG = (3, 5, 7)


def fused(comm, *args):
    any_, vmem = pl.BlockSpec(memory_space=pl.ANY), pl.BlockSpec(memory_space=pltpu.VMEM)
    V, DMA = pltpu.VMEM, pltpu.SemaphoreType.DMA
    scratch = [
        V((ROWS, 2 * FL), BF16), V((FL, ROWS), BF16),
        V((BLK, D), BF16), V((BLK, FL), BF16), V((BLK, FL), BF16), V((ROWS, 512), BF16), V((ROWS, 512), BF16),
        V((NBUF, HALF, TILE), F32), V((2, HALF, TILE), BF16), V((NIN, HALF, TILE), BF16),
        DMA((4,)), DMA((6,)), DMA((8,)), DMA((8,)),
        DMA((2,)), DMA((NIN,)), DMA((NU,)), DMA((NU,)), DMA((NU,)), DMA((1,)), DMA((1,)), DMA((1,)),
        pltpu.SemaphoreType.REGULAR, pltpu.SemaphoreType.REGULAR, pltpu.SemaphoreType.REGULAR,
    ]
    held = pl.pallas_call(
        functools.partial(kernel, comm),
        out_shape=tuple(pltpu.VMEM(s, BF16) for s in SHAPES),
        in_specs=[any_] * 7,
        out_specs=(vmem,) * 4,
        scratch_shapes=scratch,
        cost_estimate=pl.CostEstimate(flops=12 * ROWS * D * FL, bytes_accessed=90_000_000, transcendentals=ROWS * FL),
        compiler_params=pltpu.CompilerParams(
            collective_id=0 if comm else None, has_side_effects=True, vmem_limit_bytes=VLIM),
    )(*args)
    return pl.pallas_call(
        write,
        out_shape=tuple(jax.ShapeDtypeStruct(s, BF16) for s in SHAPES),
        in_specs=[vmem] * 4,
        out_specs=(any_,) * 4,
        scratch_shapes=[DMA((4, 4))],
        compiler_params=pltpu.CompilerParams(vmem_limit_bytes=1 << 20),
    )(*held)


VLIM = (64 << 20) - (64 << 10) - 2 * ROWS * D - 6 * D * FL


def solution(mesh, comm=True):
    tokens, columns, rows = P("dp", None), P(None, "tp"), P("tp", None)
    return jax.shard_map(
        functools.partial(fused, comm),
        mesh=mesh,
        in_specs=(tokens, tokens, P("dp", "tp"), P("dp", "tp"), columns, columns, rows),
        out_specs=(tokens, P("dp", "tp"), P("dp", "tp"), P(("dp", "tp"), None)),
        check_vma=False,
    )
```

```python
import functools

import jax
import jax.numpy as jnp
from jax import lax
from jax.experimental import pallas as pl
from jax.experimental.pallas import tpu as pltpu
from jax.sharding import PartitionSpec as P

MESH = pl.DeviceIdType.MESH
F32, BF16 = jnp.float32, jnp.bfloat16
ROWS, D, FL = 2048, 3072, 1024
BLK, HALF, TILE, CT = 512, 256, 512, 256
NB, NJ = ROWS // BLK, D // TILE
NT_, NU = NB * NJ, NB * (D // CT)
PER = TILE // CT
NIN, NBUF = 4, 14
NT = (((1,), (1,)), ((), ()))
NN = (((1,), (0,)), ((), ()))


def dot(a, b, dims):
    return lax.dot_general(a, b, dims, preferred_element_type=F32)


def m(i, n):
    return pl.multiple_of(i * n, n)


def kernel(comm, x, dy, gate, up, wg, wu, wd, dx, dwg, dwu, dwd,
           dgu, hid, dyb, gb, ub, xv, yv, B, d_out, d_in,
           w_sem, in_sem, x_sem, y_sem,
           d_send, d_recv, s1, r1, r2, s3, s4, r4, credit, g_credit, f_credit):
    tp = lax.axis_index("tp")
    z, c = tp // 2, lax.rem(tp, 2)
    inner = jnp.logical_and(z >= 1, z <= 2)
    outer = jnp.logical_not(inner)
    sib = z * 2 + (1 - c)
    line = jnp.where(z == 0, 1, jnp.where(z == 1, 0, jnp.where(z == 2, 3, 2))) * 2 + c
    mid = (3 - z) * 2 + c

    def loads(b, pairs):
        out = []
        for h in range(2):
            src = pl.multiple_of(b * BLK + (c if h == 0 else 1 - c) * HALF, HALF)
            rows, dst = pl.ds(src, HALF), pl.ds(h * HALF, HALF)
            for i, src_ref, dst_ref in pairs:
                out.append(pltpu.make_async_copy(src_ref.at[rows, :], dst_ref.at[dst, :], in_sem.at[i + h]))
        return out

    def dy_loads(b):
        return loads(b, [(0, dy, dyb)])

    def gu_loads(b):
        return loads(b, [(2, gate, gb), (4, up, ub)])

    def wd_load(n):
        rows = pl.ds(m(n, 512), 512)
        return pltpu.make_async_copy(wd.at[rows, :], dwd.at[rows, :], w_sem.at[n])

    wg_load = pltpu.make_async_copy(wg, dwg, w_sem.at[2])
    wu_load = pltpu.make_async_copy(wu, dwu, w_sem.at[3])
    for cp in dy_loads(0) + [wd_load(0)] + gu_loads(0):
        cp.start()

    if comm:
        barrier = pltpu.get_barrier_semaphore()
        pl.semaphore_signal(barrier, inc=1, device_id={"tp": sib}, device_id_type=MESH)
        pl.semaphore_signal(barrier, inc=1, device_id={"tp": line}, device_id_type=MESH)

        @pl.when(inner)
        def _():
            pl.semaphore_signal(barrier, inc=1, device_id={"tp": mid}, device_id_type=MESH)
            pl.semaphore_wait(barrier, 3)

        @pl.when(outer)
        def _():
            pl.semaphore_wait(barrier, 2)

    def remote(src, dst, send, recv, to):
        return pltpu.make_async_remote_copy(
            src_ref=src, dst_ref=dst, send_sem=send, recv_sem=recv, device_id={"tp": to}, device_id_type=MESH)

    def at(u, core):
        n = D // CT
        b, j = u // n, lax.rem(u, n)
        return pl.ds(pl.multiple_of(b * BLK + core * HALF, HALF), HALF), pl.ds(m(j, CT), CT)

    def mine(u):
        return dx.at[*at(u, c)]

    def theirs(u):
        return dx.at[*at(u, 1 - c)]

    def d_copy(t):
        return remote(d_out.at[lax.rem(t, 2)], d_in.at[lax.rem(t, NIN)], d_send.at[lax.rem(t, 2)],
                      d_recv.at[lax.rem(t, NIN)], sib)

    def p_copy(u):
        return remote(mine(u), mine(u), s1.at[u], r1.at[u], line)

    def q_copy(u):
        return remote(mine(u), theirs(u), s1.at[u], r2.at[u], mid)

    def f_copy(u):
        return remote(mine(u), mine(u), s3.at[0], r2.at[u], line)

    def g_copy(u):
        return remote(mine(u), mine(u), s4.at[0], r4.at[0], sib)

    def pending(u):
        i = lax.rem(u, PER)
        return lax.rem(u // PER, NBUF), slice(None), pl.ds(m(i, CT), CT)

    def take_sibling(t):
        d_copy(t).wait_recv()
        b, j = t // NJ, lax.rem(t, NJ)
        total = B[lax.rem(t, NBUF)] + d_in[lax.rem(t, NIN)].astype(F32)

        @pl.when(outer)
        def _():
            dx[pl.ds(pl.multiple_of(b * BLK + c * HALF, HALF), HALF), pl.ds(m(j, TILE), TILE)] = total.astype(BF16)
            for i in range(PER):
                p_copy(t * PER + i).start()

        @pl.when(inner)
        def _():
            B[lax.rem(t, NBUF)] = total

        @pl.when(t < NT_ - NIN)
        def _():
            pl.semaphore_signal(credit, inc=1, device_id={"tp": sib}, device_id_type=MESH)

    def inner_sum(u):
        p_copy(u).wait_recv()
        p = at(u, c)
        dx[*p] = (B[*pending(u)] + dx[*p].astype(F32)).astype(BF16)
        q_copy(u).start()

    def final_sum(u):
        q_copy(u).wait_recv()
        q_copy(u).wait_send()
        p = at(u, c)
        dx[*p] = (dx[*p].astype(F32) + dx[*at(u, 1 - c)].astype(F32)).astype(BF16)
        pl.semaphore_signal(g_credit, inc=1, device_id={"tp": sib}, device_id_type=MESH)
        pl.semaphore_wait(f_credit, 1)
        f_copy(u).start()
        pl.semaphore_wait(g_credit, 1)
        g_copy(u).start()

    def release(u):
        p_copy(u).wait_send()
        pl.semaphore_signal(f_credit, inc=1, device_id={"tp": line}, device_id_type=MESH)

    def forward(u):
        f_copy(u).wait_recv()
        g_copy(u).start()

    def tick(h):
        if not comm:
            return

        @pl.when(jnp.logical_and(inner, jnp.logical_and(h >= LAG[0], h < NU + LAG[0])))
        def _():
            inner_sum(h - LAG[0])

        @pl.when(jnp.logical_and(inner, jnp.logical_and(h >= LAG[1], h < NU + LAG[1])))
        def _():
            final_sum(h - LAG[1])

        @pl.when(jnp.logical_and(outer, jnp.logical_and(h >= LAG[0], h < NU + LAG[0])))
        def _():
            release(h - LAG[0])

        @pl.when(jnp.logical_and(outer, jnp.logical_and(h >= LAG[2], h < NU + LAG[2])))
        def _():
            forward(h - LAG[2])

    def tile_copies(src, dst, i, sem):
        cols = pl.ds(m(i, 512), 512)
        return [
            pltpu.make_async_copy(
                src.at[pl.ds(pl.multiple_of(b * BLK + (c if h == 0 else 1 - c) * HALF, HALF), HALF), cols],
                dst.at[pl.ds(b * BLK + h * HALF, HALF), :],
                sem.at[2 * b + h],
            )
            for b in range(NB)
            for h in range(2)
        ]

    def block(b, _):
        for cp in dy_loads(b):
            cp.wait()
        rows = pl.ds(m(b, BLK), BLK)

        def hidden(n, _):
            @pl.when(b == 0)
            def _():
                wd_load(n).wait()

                @pl.when(n == 0)
                def _():
                    wd_load(1).start()
                    wg_load.start()
                    wu_load.start()

            cols = pl.ds(m(n, 512), 512)
            dh = dot(dyb[...], dwd[cols, :], NT)

            @pl.when(n == 0)
            def _():
                for cp in gu_loads(b):
                    cp.wait()

            g, u = gb[:, cols].astype(F32), ub[:, cols].astype(F32)
            s = jax.nn.sigmoid(g)
            gs = g * s
            dgu[rows, cols] = (dh * u * (s * (1.0 + g * (1.0 - s)))).astype(BF16)
            dgu[rows, pl.ds(pl.multiple_of(FL + n * 512, 512), 512)] = (dh * gs).astype(BF16)
            hid[cols, rows] = (gs * u).T.astype(BF16)
            tick(8 * b + n)
            return 0

        lax.fori_loop(0, FL // 512, hidden, 0)

        @pl.when(b < NB - 1)
        def _():
            for cp in dy_loads(b + 1) + gu_loads(b + 1):
                cp.start()

        @pl.when(b == 0)
        def _():
            wg_load.wait()
            wu_load.wait()
            for cp in tile_copies(x, xv, 0, x_sem) + tile_copies(dy, yv, 0, y_sem):
                cp.start()

        def tile(j, _):
            t = b * NJ + j
            if comm:
                @pl.when(t >= 2)
                def _():
                    d_copy(t - 2).wait_send()
            cols = pl.ds(m(j, TILE), TILE)
            v = dot(dgu[rows, pl.ds(0, FL)], dwg[cols, :], NT) + dot(dgu[rows, pl.ds(FL, FL)], dwu[cols, :], NT)
            B[lax.rem(t, NBUF)] = v[:HALF]
            d_out[lax.rem(t, 2)] = v[HALF:].astype(BF16)
            if comm:
                @pl.when(t >= NIN)
                def _():
                    pl.semaphore_wait(credit, 1)
                d_copy(t).start()

                @pl.when(t >= 1)
                def _():
                    take_sibling(t - 1)

                tick(8 * b + 2 + j)
            return 0

        lax.fori_loop(0, NJ, tile, 0)
        return 0

    lax.fori_loop(0, NB, block, 0)
    if comm:
        take_sibling(NT_ - 1)

    NI = D // 512
    xt = dyb.at[:, pl.ds(0, ROWS)]

    def grads(i, _):
        for cp in tile_copies(x, xv, i, x_sem):
            cp.wait()

        def flip(r, _):
            rows = pl.ds(m(r, 512), 512)
            xt[:, rows] = xv[rows, :].T
            return 0

        lax.fori_loop(0, ROWS // 512, flip, 0)
        tick(8 * NB + 4 * i)

        @pl.when(i + 1 < NI)
        def _():
            for cp in tile_copies(x, xv, i + 1, x_sem):
                cp.start()

        out = pl.ds(m(i, 512), 512)

        def gu(n, _):
            cols = pl.ds(m(n, 512), 512)
            dwg[out, cols] = dot(xt[...], dgu[:, cols], NN).astype(BF16)
            dwu[out, cols] = dot(xt[...], dgu[:, pl.ds(pl.multiple_of(FL + n * 512, 512), 512)], NN).astype(BF16)
            tick(8 * NB + 4 * i + 1 + n)
            return 0

        lax.fori_loop(0, 2, gu, 0)
        for cp in tile_copies(dy, yv, i, y_sem):
            cp.wait()

        def down(n, _):
            rows = pl.ds(m(n, 512), 512)
            dwd[rows, out] = dot(hid[rows, :], yv[...], NN).astype(BF16)
            return 0

        lax.fori_loop(0, 2, down, 0)
        tick(8 * NB + 4 * i + 3)

        @pl.when(i + 1 < NI)
        def _():
            for cp in tile_copies(dy, yv, i + 1, y_sem):
                cp.start()
        return 0

    lax.fori_loop(0, NI, grads, 0)

    if comm:
        def drain(h, _):
            tick(h)
            return 0

        lax.fori_loop(8 * NB + 4 * NI, NU + LAG[2], drain, 0)
        d_copy(NT_ - 2).wait_send()
        d_copy(NT_ - 1).wait_send()
        half = dx.at[pl.ds(0, ROWS // 2), :]
        remote(half, half, s4.at[0], r4.at[0], sib).wait()

        @pl.when(inner)
        def _():
            remote(half, half, s3.at[0], r2.at[0], line).wait_send()


def write(*refs):
    n = len(refs) // 2
    sem, refs = refs[-1], refs[:-1]
    copies = []
    for i in range(n):
        src, dst = refs[i], refs[n + i]
        rows = src.shape[0] // 4
        for k in range(4):
            part = pl.ds(k * rows, rows)
            copies.append(pltpu.make_async_copy(src.at[part, :], dst.at[part, :], sem.at[i, k]))
    for cp in copies:
        cp.start()
    for cp in copies:
        cp.wait()


SHAPES = ((ROWS, D), (D, FL), (D, FL), (FL, D))
LAG = (5, 7, 9)


def fused(comm, *args):
    any_, vmem = pl.BlockSpec(memory_space=pl.ANY), pl.BlockSpec(memory_space=pltpu.VMEM)
    V, DMA = pltpu.VMEM, pltpu.SemaphoreType.DMA
    scratch = [
        V((ROWS, 2 * FL), BF16), V((FL, ROWS), BF16),
        V((BLK, D), BF16), V((BLK, FL), BF16), V((BLK, FL), BF16), V((ROWS, 512), BF16), V((ROWS, 512), BF16),
        V((NBUF, HALF, TILE), F32), V((2, HALF, TILE), BF16), V((NIN, HALF, TILE), BF16),
        DMA((4,)), DMA((6,)), DMA((8,)), DMA((8,)),
        DMA((2,)), DMA((NIN,)), DMA((NU,)), DMA((NU,)), DMA((NU,)), DMA((1,)), DMA((1,)), DMA((1,)),
        pltpu.SemaphoreType.REGULAR, pltpu.SemaphoreType.REGULAR, pltpu.SemaphoreType.REGULAR,
    ]
    held = pl.pallas_call(
        functools.partial(kernel, comm),
        out_shape=tuple(pltpu.VMEM(s, BF16) for s in SHAPES),
        in_specs=[any_] * 7,
        out_specs=(vmem,) * 4,
        scratch_shapes=scratch,
        cost_estimate=pl.CostEstimate(flops=12 * ROWS * D * FL, bytes_accessed=90_000_000, transcendentals=ROWS * FL),
        compiler_params=pltpu.CompilerParams(
            collective_id=0 if comm else None, has_side_effects=True, vmem_limit_bytes=VLIM),
    )(*args)
    return pl.pallas_call(
        write,
        out_shape=tuple(jax.ShapeDtypeStruct(s, BF16) for s in SHAPES),
        in_specs=[vmem] * 4,
        out_specs=(any_,) * 4,
        scratch_shapes=[DMA((4, 4))],
        compiler_params=pltpu.CompilerParams(vmem_limit_bytes=1 << 20),
    )(*held)


VLIM = (64 << 20) - (64 << 10) - 2 * ROWS * D - 6 * D * FL


def solution(mesh, comm=True):
    tokens, columns, rows = P("dp", None), P(None, "tp"), P("tp", None)
    return jax.shard_map(
        functools.partial(fused, comm),
        mesh=mesh,
        in_specs=(tokens, tokens, P("dp", "tp"), P("dp", "tp"), columns, columns, rows),
        out_specs=(tokens, P("dp", "tp"), P("dp", "tp"), P(("dp", "tp"), None)),
        check_vma=False,
    )
```

```python
import functools

import jax
import jax.numpy as jnp
from jax import lax
from jax.experimental import pallas as pl
from jax.experimental.pallas import tpu as pltpu
from jax.sharding import PartitionSpec as P

MESH = pl.DeviceIdType.MESH
F32, BF16 = jnp.float32, jnp.bfloat16
ROWS, D, FL = 2048, 3072, 1024
BLK, HALF, TILE, CT = 512, 256, 512, 256
NB, NJ = ROWS // BLK, D // TILE
NT_, NU = NB * NJ, NB * (D // CT)
PER = TILE // CT
NIN, NBUF = 4, 11
NT = (((1,), (1,)), ((), ()))
NN = (((1,), (0,)), ((), ()))


def dot(a, b, dims):
    return lax.dot_general(a, b, dims, preferred_element_type=F32)


def m(i, n):
    return pl.multiple_of(i * n, n)


def kernel(comm, x, dy, gate, up, wg, wu, wd, dx, dwg, dwu, dwd,
           dgu, hid, dyb, gb, ub, xv, yv, B, d_out, d_in,
           w_sem, k_sem, in_sem, x_sem, y_sem,
           d_send, d_recv, s1, r1, r2, s3, s4, r4, credit, g_credit, f_credit):
    tp = lax.axis_index("tp")
    z, c = tp // 2, lax.rem(tp, 2)
    inner = jnp.logical_and(z >= 1, z <= 2)
    outer = jnp.logical_not(inner)
    sib = z * 2 + (1 - c)
    line = jnp.where(z == 0, 1, jnp.where(z == 1, 0, jnp.where(z == 2, 3, 2))) * 2 + c
    mid = (3 - z) * 2 + c

    def loads(b, pairs):
        out = []
        for h in range(2):
            src = pl.multiple_of(b * BLK + (c if h == 0 else 1 - c) * HALF, HALF)
            rows, dst = pl.ds(src, HALF), pl.ds(h * HALF, HALF)
            for i, src_ref, dst_ref in pairs:
                out.append(pltpu.make_async_copy(src_ref.at[rows, :], dst_ref.at[dst, :], in_sem.at[i + h]))
        return out

    def dy_loads(b):
        return loads(b, [(0, dy, dyb)])

    def first_loads(k):
        cols = pl.ds(k * (D // 2), D // 2)
        out = [pltpu.make_async_copy(wd.at[pl.ds(0, 512), cols], dwd.at[pl.ds(0, 512), cols], k_sem.at[k, 2])]
        for h in range(2):
            src = pl.ds(pl.multiple_of((c if h == 0 else 1 - c) * HALF, HALF), HALF)
            out.append(pltpu.make_async_copy(dy.at[src, cols], dyb.at[pl.ds(h * HALF, HALF), cols], k_sem.at[k, h]))
        return out

    def gu_loads(b):
        return loads(b, [(2, gate, gb), (4, up, ub)])

    def wd_load(n):
        rows = pl.ds(m(n, 512), 512)
        return pltpu.make_async_copy(wd.at[rows, :], dwd.at[rows, :], w_sem.at[n])

    wg_load = pltpu.make_async_copy(wg, dwg, w_sem.at[2])
    wu_load = pltpu.make_async_copy(wu, dwu, w_sem.at[3])
    for cp in first_loads(0) + first_loads(1) + gu_loads(0):
        cp.start()

    if comm:
        barrier = pltpu.get_barrier_semaphore()
        pl.semaphore_signal(barrier, inc=1, device_id={"tp": sib}, device_id_type=MESH)
        pl.semaphore_signal(barrier, inc=1, device_id={"tp": line}, device_id_type=MESH)

        @pl.when(inner)
        def _():
            pl.semaphore_signal(barrier, inc=1, device_id={"tp": mid}, device_id_type=MESH)

    def enter():
        @pl.when(inner)
        def _():
            pl.semaphore_wait(barrier, 3)

        @pl.when(outer)
        def _():
            pl.semaphore_wait(barrier, 2)

    def remote(src, dst, send, recv, to):
        return pltpu.make_async_remote_copy(
            src_ref=src, dst_ref=dst, send_sem=send, recv_sem=recv, device_id={"tp": to}, device_id_type=MESH)

    def at(u, core):
        n = D // CT
        b, j = u // n, lax.rem(u, n)
        return pl.ds(pl.multiple_of(b * BLK + core * HALF, HALF), HALF), pl.ds(m(j, CT), CT)

    def mine(u):
        return dx.at[*at(u, c)]

    def theirs(u):
        return dx.at[*at(u, 1 - c)]

    def d_copy(t):
        return remote(d_out.at[lax.rem(t, 2)], d_in.at[lax.rem(t, NIN)], d_send.at[lax.rem(t, 2)],
                      d_recv.at[lax.rem(t, NIN)], sib)

    def p_copy(u):
        return remote(mine(u), mine(u), s1.at[u], r1.at[u], line)

    def q_copy(u):
        return remote(mine(u), theirs(u), s1.at[u], r2.at[u], mid)

    def f_copy(u):
        return remote(mine(u), mine(u), s3.at[0], r2.at[u], line)

    def g_copy(u):
        return remote(mine(u), mine(u), s4.at[0], r4.at[0], sib)

    def pending(u):
        i = lax.rem(u, PER)
        return lax.rem(u // PER, NBUF), slice(None), pl.ds(m(i, CT), CT)

    def take_sibling(t):
        d_copy(t).wait_recv()
        b, j = t // NJ, lax.rem(t, NJ)
        total = B[lax.rem(t, NBUF)] + d_in[lax.rem(t, NIN)].astype(F32)

        @pl.when(outer)
        def _():
            dx[pl.ds(pl.multiple_of(b * BLK + c * HALF, HALF), HALF), pl.ds(m(j, TILE), TILE)] = total.astype(BF16)
            for i in range(PER):
                p_copy(t * PER + i).start()

        @pl.when(inner)
        def _():
            B[lax.rem(t, NBUF)] = total

        @pl.when(t < NT_ - NIN)
        def _():
            pl.semaphore_signal(credit, inc=1, device_id={"tp": sib}, device_id_type=MESH)

    def inner_sum(u):
        p_copy(u).wait_recv()
        p = at(u, c)
        dx[*p] = (B[*pending(u)] + dx[*p].astype(F32)).astype(BF16)
        q_copy(u).start()

    def final_sum(u):
        q_copy(u).wait_recv()
        q_copy(u).wait_send()
        p = at(u, c)
        dx[*p] = (dx[*p].astype(F32) + dx[*at(u, 1 - c)].astype(F32)).astype(BF16)
        pl.semaphore_signal(g_credit, inc=1, device_id={"tp": sib}, device_id_type=MESH)
        pl.semaphore_wait(f_credit, 1)
        f_copy(u).start()
        pl.semaphore_wait(g_credit, 1)
        g_copy(u).start()

    def release(u):
        p_copy(u).wait_send()
        pl.semaphore_signal(f_credit, inc=1, device_id={"tp": line}, device_id_type=MESH)

    def forward(u):
        f_copy(u).wait_recv()
        g_copy(u).start()

    def tick(h):
        if not comm:
            return

        @pl.when(jnp.logical_and(inner, jnp.logical_and(h >= LAG[1], h < NU + LAG[1])))
        def _():
            final_sum(h - LAG[1])

        @pl.when(jnp.logical_and(inner, jnp.logical_and(h >= LAG[0], h < NU + LAG[0])))
        def _():
            inner_sum(h - LAG[0])

        @pl.when(jnp.logical_and(outer, jnp.logical_and(h >= LAG[0], h < NU + LAG[0])))
        def _():
            release(h - LAG[0])

        @pl.when(jnp.logical_and(outer, jnp.logical_and(h >= LAG[2], h < NU + LAG[2])))
        def _():
            forward(h - LAG[2])

    def tile_copies(src, dst, i, sem):
        cols = pl.ds(m(i, 512), 512)
        return [
            pltpu.make_async_copy(
                src.at[pl.ds(pl.multiple_of(b * BLK + (c if h == 0 else 1 - c) * HALF, HALF), HALF), cols],
                dst.at[pl.ds(b * BLK + h * HALF, HALF), :],
                sem.at[2 * b + h],
            )
            for b in range(NB)
            for h in range(2)
        ]

    def hidden(b, n, dh):
        cols, rows = pl.ds(m(n, 512), 512), pl.ds(m(b, BLK), BLK)
        g, u = gb[:, cols].astype(F32), ub[:, cols].astype(F32)
        s = jax.nn.sigmoid(g)
        gs = g * s
        dgu[rows, cols] = (dh * u * (s * (1.0 + g * (1.0 - s)))).astype(BF16)
        dgu[rows, pl.ds(pl.multiple_of(FL + n * 512, 512), 512)] = (dh * gs).astype(BF16)
        hid[cols, rows] = (gs * u).T.astype(BF16)

    def block(b, _):
        rows = pl.ds(m(b, BLK), BLK)

        @pl.when(b > 0)
        def _():
            for cp in dy_loads(b) + gu_loads(b):
                cp.wait()

            def step(n, _):
                hidden(b, n, dot(dyb[...], dwd[pl.ds(m(n, 512), 512), :], NT))
                tick(8 * b + n)
                return 0

            lax.fori_loop(0, FL // 512, step, 0)

        @pl.when(b < NB - 1)
        def _():
            for cp in dy_loads(b + 1) + gu_loads(b + 1):
                cp.start()

        @pl.when(b == 0)
        def _():
            wg_load.wait()
            wu_load.wait()
            for cp in tile_copies(x, xv, 0, x_sem) + tile_copies(dy, yv, 0, y_sem):
                cp.start()

        def tile(j, _):
            t = b * NJ + j
            if comm:
                @pl.when(t >= 2)
                def _():
                    d_copy(t - 2).wait_send()
            cols = pl.ds(m(j, TILE), TILE)
            v = dot(dgu[rows, pl.ds(0, FL)], dwg[cols, :], NT) + dot(dgu[rows, pl.ds(FL, FL)], dwu[cols, :], NT)
            B[lax.rem(t, NBUF)] = v[:HALF]
            d_out[lax.rem(t, 2)] = v[HALF:].astype(BF16)
            if comm:
                @pl.when(t >= NIN)
                def _():
                    pl.semaphore_wait(credit, 1)
                d_copy(t).start()

                @pl.when(t >= 1)
                def _():
                    take_sibling(t - 1)

                tick(8 * b + 2 + j)
            return 0

        lax.fori_loop(0, NJ, tile, 0)
        return 0

    for cp in first_loads(0):
        cp.wait()
    wd_load(1).start()
    wg_load.start()
    wu_load.start()
    lo, hi = pl.ds(0, D // 2), pl.ds(D // 2, D // 2)

    def first(n, _):
        @pl.when(n == 1)
        def _():
            wd_load(1).wait()

        rows = pl.ds(m(n, 512), 512)
        dh = dot(dyb[:, lo], dwd[rows, lo], NT)

        @pl.when(n == 0)
        def _():
            for cp in first_loads(1) + gu_loads(0):
                cp.wait()

        hidden(0, n, dh + dot(dyb[:, hi], dwd[rows, hi], NT))
        return 0

    lax.fori_loop(0, FL // 512, first, 0)
    if comm:
        enter()
    lax.fori_loop(0, NB, block, 0)
    if comm:
        take_sibling(NT_ - 1)

    NI = D // 512
    xt = dyb.at[:, pl.ds(0, ROWS)]

    def grads(i, _):
        for cp in tile_copies(x, xv, i, x_sem):
            cp.wait()

        def flip(r, _):
            rows = pl.ds(m(r, 512), 512)
            xt[:, rows] = xv[rows, :].T
            return 0

        lax.fori_loop(0, ROWS // 512, flip, 0)
        tick(8 * NB + 4 * i)

        @pl.when(i + 1 < NI)
        def _():
            for cp in tile_copies(x, xv, i + 1, x_sem):
                cp.start()

        out = pl.ds(m(i, 512), 512)

        def gu(n, _):
            cols = pl.ds(m(n, 512), 512)
            dwg[out, cols] = dot(xt[...], dgu[:, cols], NN).astype(BF16)
            dwu[out, cols] = dot(xt[...], dgu[:, pl.ds(pl.multiple_of(FL + n * 512, 512), 512)], NN).astype(BF16)
            tick(8 * NB + 4 * i + 1 + n)
            return 0

        lax.fori_loop(0, 2, gu, 0)
        for cp in tile_copies(dy, yv, i, y_sem):
            cp.wait()

        def down(n, _):
            rows = pl.ds(m(n, 512), 512)
            dwd[rows, out] = dot(hid[rows, :], yv[...], NN).astype(BF16)
            return 0

        lax.fori_loop(0, 2, down, 0)
        tick(8 * NB + 4 * i + 3)

        @pl.when(i + 1 < NI)
        def _():
            for cp in tile_copies(dy, yv, i + 1, y_sem):
                cp.start()
        return 0

    lax.fori_loop(0, NI, grads, 0)

    if comm:
        def drain(h, _):
            tick(h)
            return 0

        lax.fori_loop(8 * NB + 4 * NI, NU + LAG[2], drain, 0)
        d_copy(NT_ - 2).wait_send()
        d_copy(NT_ - 1).wait_send()
        half = dx.at[pl.ds(0, ROWS // 2), :]
        remote(half, half, s4.at[0], r4.at[0], sib).wait()

        @pl.when(inner)
        def _():
            remote(half, half, s3.at[0], r2.at[0], line).wait_send()


def write(*refs):
    n = len(refs) // 2
    sem, refs = refs[-1], refs[:-1]
    copies = []
    for i in range(n):
        src, dst = refs[i], refs[n + i]
        rows = src.shape[0] // 4
        for k in range(4):
            part = pl.ds(k * rows, rows)
            copies.append(pltpu.make_async_copy(src.at[part, :], dst.at[part, :], sem.at[i, k]))
    for cp in copies:
        cp.start()
    for cp in copies:
        cp.wait()


SHAPES = ((ROWS, D), (D, FL), (D, FL), (FL, D))
LAG = (5, 7, 9)


def fused(comm, *args):
    any_, vmem = pl.BlockSpec(memory_space=pl.ANY), pl.BlockSpec(memory_space=pltpu.VMEM)
    V, DMA = pltpu.VMEM, pltpu.SemaphoreType.DMA
    scratch = [
        V((ROWS, 2 * FL), BF16), V((FL, ROWS), BF16),
        V((BLK, D), BF16), V((BLK, FL), BF16), V((BLK, FL), BF16), V((ROWS, 512), BF16), V((ROWS, 512), BF16),
        V((NBUF, HALF, TILE), F32), V((2, HALF, TILE), BF16), V((NIN, HALF, TILE), BF16),
        DMA((4,)), DMA((2, 3)), DMA((6,)), DMA((8,)), DMA((8,)),
        DMA((2,)), DMA((NIN,)), DMA((NU,)), DMA((NU,)), DMA((NU,)), DMA((1,)), DMA((1,)), DMA((1,)),
        pltpu.SemaphoreType.REGULAR, pltpu.SemaphoreType.REGULAR, pltpu.SemaphoreType.REGULAR,
    ]
    held = pl.pallas_call(
        functools.partial(kernel, comm),
        out_shape=tuple(pltpu.VMEM(s, BF16) for s in SHAPES),
        in_specs=[any_] * 7,
        out_specs=(vmem,) * 4,
        scratch_shapes=scratch,
        cost_estimate=pl.CostEstimate(flops=12 * ROWS * D * FL, bytes_accessed=90_000_000, transcendentals=ROWS * FL),
        compiler_params=pltpu.CompilerParams(
            collective_id=0 if comm else None, has_side_effects=True, vmem_limit_bytes=VLIM),
    )(*args)
    return pl.pallas_call(
        write,
        out_shape=tuple(jax.ShapeDtypeStruct(s, BF16) for s in SHAPES),
        in_specs=[vmem] * 4,
        out_specs=(any_,) * 4,
        scratch_shapes=[DMA((4, 4))],
        compiler_params=pltpu.CompilerParams(vmem_limit_bytes=1 << 20),
    )(*held)


VLIM = (64 << 20) - (64 << 10) - 2 * ROWS * D - 6 * D * FL


def solution(mesh, comm=True):
    tokens, columns, rows = P("dp", None), P(None, "tp"), P("tp", None)
    return jax.shard_map(
        functools.partial(fused, comm),
        mesh=mesh,
        in_specs=(tokens, tokens, P("dp", "tp"), P("dp", "tp"), columns, columns, rows),
        out_specs=(tokens, P("dp", "tp"), P("dp", "tp"), P(("dp", "tp"), None)),
        check_vma=False,
    )
```
